32 devices in a mesh: row: 4 (over z), col: 8 (over y, x, core).
Axes of the slice: x: 2, y: 2, z: 4, core: 2. Of those that a mesh axis runs over, the one named last changes fastest.
Arguments:
- reflection: bfloat16 [2, 1024, 8192], P(None, 'col', 'row'), may hold values from -6 to 6
- focus_in: bfloat16 [2, 8192, 8192], P(None, 'row', 'col'), may hold values from -1 to 1
- focus_out: bfloat16 [2, 8192, 1024], P(None, 'row'), may hold values from -1 to 1
- ref_angle: float32 [8192, 8192], P('row', 'col'), may hold values from -3.140625 to 3.140625
- element_order: int32 [8192], P('row'), may hold values from 0 to 8191, as said below
- q_start: bfloat16 [8192, 2, 256], P('row'), may hold values from -1 to 1
Outputs:
- basis: float32 [8192, 2, 256], P(('row', 'col'))
The draws below stay inside these ranges and needn't reach their ends.
Inputs may be any that keep to these rules, and one draw needn't show every extreme that they name: `element_order`: a permutation of 0 to 8191 that maps each aligned block of 512 positions onto the same block.
All inputs are finite; a program needn't handle non-finite values.
Results may differ from the reference program's by a relative error of at most 0.0047.
Values may be sent and summed in bfloat16 or wider, within the bound.
No kernel may reach another device: no remote copies, remote signals or barrier semaphores. Data moves between devices by JAX's collectives and lax.ppermute only.
A program may use at most 192 MiB of HBM per device.

```python
import math
import jax
import jax.numpy as jnp
from jax import lax

NF = 8192
RANK = 256
PANEL_W = 512
OUT_TRANS = 1024
IN_TRANS = 8192


def draw_element_order(key, part):
    blocks = IN_TRANS // PANEL_W
    keys = jax.random.split(jax.random.fold_in(key, 17), blocks)
    shuffled = jax.vmap(lambda single: jax.random.permutation(single, PANEL_W))(keys)
    offsets = (jnp.arange(blocks, dtype=jnp.int32) * PANEL_W)[:, None]
    return (shuffled.astype(jnp.int32) + offsets).reshape(-1).astype(jnp.int32)


def drawn_field(key, shape, scale):
    values = jax.random.truncated_normal(key, -6.0, 6.0, shape, jnp.float32)
    return (values * scale).astype(jnp.bfloat16)


def draw_reflection(key, part):
    return drawn_field(jax.random.fold_in(key, 31), (2, OUT_TRANS, IN_TRANS), 1.0)


def draw_focus_in(key, part):
    return drawn_field(jax.random.fold_in(key, 37), (2, IN_TRANS, NF), IN_TRANS ** (-0.5))


def draw_focus_out(key, part):
    return drawn_field(jax.random.fold_in(key, 41), (2, NF, OUT_TRANS), OUT_TRANS ** (-0.5))


def draw_q_start(key, part):
    return drawn_field(jax.random.fold_in(key, 43), (NF, 2, RANK), NF ** (-0.5))


def setup_inputs(seed: int = 0) -> dict:
    arg_keys = jax.random.split(jax.random.key(seed), 7)
    reflection = draw_reflection(jax.random.fold_in(arg_keys[6], 71), 0)
    focus_in = draw_focus_in(jax.random.fold_in(arg_keys[6], 71), 0)
    focus_out = draw_focus_out(jax.random.fold_in(arg_keys[6], 71), 0)
    ref_angle = jnp.clip(jax.random.uniform(arg_keys[3], (NF, NF), jnp.float32, -3.140625, 3.140625), -3.140625, 3.140625)
    element_order = draw_element_order(jax.random.fold_in(arg_keys[6], 71), 0)
    q_start = draw_q_start(jax.random.fold_in(arg_keys[6], 71), 0)
    return dict(reflection=reflection, focus_in=focus_in, focus_out=focus_out, ref_angle=ref_angle, element_order=element_order, q_start=q_start)


def cross(left_re, left_im, right_re, right_im):
    real_part = jnp.dot(left_re, right_re, preferred_element_type=jnp.float32) - jnp.dot(left_im, right_im, preferred_element_type=jnp.float32)
    imag_part = jnp.dot(left_re, right_im, preferred_element_type=jnp.float32) + jnp.dot(left_im, right_re, preferred_element_type=jnp.float32)
    return (real_part, imag_part)

def tdot(left, right, precision=None):
    return lax.dot_general(left, right, (((0,), (0,)), ((), ())), precision=precision, preferred_element_type=jnp.float32)

def adjoint_product(left_re, left_im, right_re, right_im, precision=None):
    real_part = tdot(left_re, right_re, precision) + tdot(left_im, right_im, precision)
    imag_part = tdot(left_re, right_im, precision) - tdot(left_im, right_re, precision)
    return (real_part, imag_part)

def complex_chol(gram_re, gram_im):
    order = gram_re.shape[0]
    positions = jnp.arange(order)
    high = lax.Precision.HIGHEST

    def step(column, carry):
        low_re, low_im = carry
        row_re = low_re[column]
        row_im = low_im[column]
        value_re = gram_re[:, column] - (jnp.dot(low_re, row_re, precision=high) + jnp.dot(low_im, row_im, precision=high))
        value_im = gram_im[:, column] - (jnp.dot(low_im, row_re, precision=high) - jnp.dot(low_re, row_im, precision=high))
        pivot = jnp.sqrt(value_re[column])
        below = positions > column
        new_re = jnp.where(below, value_re / pivot, jnp.where(positions == column, pivot, jnp.zeros_like(pivot)))
        new_im = jnp.where(below, value_im / pivot, jnp.zeros_like(pivot))
        return (low_re.at[:, column].set(new_re), low_im.at[:, column].set(new_im))
    start = (jnp.zeros((order, order), jnp.float32), jnp.zeros((order, order), jnp.float32))
    return lax.fori_loop(0, order, step, start)

def lower_inverse(low_re, low_im):
    order = low_re.shape[0]
    positions = jnp.arange(order)
    high = lax.Precision.HIGHEST

    def step(column, carry):
        inv_re, inv_im = carry
        row_re = low_re[column]
        row_im = low_im[column]
        sum_re = jnp.dot(row_re, inv_re, precision=high) - jnp.dot(row_im, inv_im, precision=high)
        sum_im = jnp.dot(row_re, inv_im, precision=high) + jnp.dot(row_im, inv_re, precision=high)
        pivot = low_re[column, column]
        unit = (positions == column).astype(jnp.float32)
        return (inv_re.at[column].set((unit - sum_re) / pivot), inv_im.at[column].set(-sum_im / pivot))
    start = (jnp.zeros((order, order), jnp.float32), jnp.zeros((order, order), jnp.float32))
    return lax.fori_loop(0, order, step, start)

def orthonormal(image_re, image_im, gram_re, gram_im, scale):
    high = lax.Precision.HIGHEST
    low_re, low_im = complex_chol(gram_re, gram_im)
    inv_re, inv_im = lower_inverse(low_re, low_im)
    basis_re = jnp.dot(image_re, inv_re.T, precision=high) + jnp.dot(image_im, inv_im.T, precision=high)
    basis_im = jnp.dot(image_im, inv_re.T, precision=high) - jnp.dot(image_re, inv_im.T, precision=high)
    return jnp.stack([basis_re, basis_im], axis=1) * scale

def reference(reflection, focus_in, focus_out, ref_angle, element_order, q_start):
    ordered = jnp.take(focus_in, element_order.astype(jnp.int32), axis=1)
    focus_re, focus_im = cross(reflection[0], reflection[1], ordered[0], ordered[1])
    focus_re = focus_re.astype(jnp.bfloat16)
    focus_im = focus_im.astype(jnp.bfloat16)
    outer_re, outer_im = cross(focus_out[0], focus_out[1], focus_re, focus_im)
    cosine = jnp.cos(ref_angle)
    sine = jnp.sin(ref_angle)
    dense_re = (outer_re * cosine + outer_im * sine).astype(jnp.bfloat16)
    dense_im = (outer_im * cosine - outer_re * sine).astype(jnp.bfloat16)
    adj_re, adj_im = adjoint_product(dense_re, dense_im, q_start[:, 0], q_start[:, 1])
    adj_re = adj_re.astype(jnp.bfloat16)
    adj_im = adj_im.astype(jnp.bfloat16)
    image_re, image_im = cross(dense_re, dense_im, adj_re, adj_im)
    gram_re, gram_im = adjoint_product(image_re, image_im, image_re, image_im, lax.Precision.HIGHEST)
    return orthonormal(image_re, image_im, gram_re, gram_im, math.sqrt(NF))
```

```python
import functools
import math

import jax
import jax.numpy as jnp
from jax import lax
from jax.experimental import pallas as pl
from jax.experimental.pallas import tpu as pltpu
from jax.sharding import PartitionSpec as P

PANEL_W = 512
FOCAL_CHUNKS = 4
HIGH = lax.Precision.HIGHEST


def dot(left, right):
    return jnp.dot(left, right, preferred_element_type=jnp.float32)


def tdot(left, right, precision=None):
    return lax.dot_general(
        left,
        right,
        (((0,), (0,)), ((), ())),
        precision=precision,
        preferred_element_type=jnp.float32,
    )


def cross(left_re, left_im, right_re, right_im):
    real_part = dot(left_re, right_re) - dot(left_im, right_im)
    imag_part = dot(left_re, right_im) + dot(left_im, right_re)
    return real_part, imag_part


def adjoint_product(left_re, left_im, right_re, right_im, precision=None):
    real_part = tdot(left_re, right_re, precision) + tdot(left_im, right_im, precision)
    imag_part = tdot(left_re, right_im, precision) - tdot(left_im, right_re, precision)
    return real_part, imag_part


def flip(value, axis, mask):
    size = lax.axis_size(axis)
    return lax.ppermute(value, axis, [(i, i ^ mask) for i in range(size)])


def line_sum(chunks, axis, delay):
    size = lax.axis_size(axis)
    place = lax.axis_index(axis)
    half = size // 2
    low = jnp.bfloat16
    if size == 1:
        return [chunk.astype(low) for chunk in chunks]
    middle = (place == half - 1) | (place == half)
    swap = [(half - 1, half), (half, half - 1)]
    if size != 4:
        results = []
        for chunk in chunks:
            for d in range(half - 1):
                hop = [(d, d + 1), (size - 1 - d, size - 2 - d)]
                chunk = chunk + lax.ppermute(chunk.astype(low), axis, hop).astype(jnp.float32)
            got = lax.ppermute(chunk.astype(low), axis, swap)
            total = (chunk + got.astype(jnp.float32)).astype(low)
            for d in reversed(range(half - 1)):
                hop = [(d + 1, d), (size - 2 - d, size - 1 - d)]
                got = lax.ppermute(total, axis, hop)
                total = jnp.where((place == d) | (place == size - 1 - d), got, total)
            results.append(total)
        return results
    count = len(chunks)
    totals = []
    results = []
    for step in range(count + delay):
        send = chunks[step].astype(low) if step < count else totals[step - delay]
        if delay <= step < count:
            send = jnp.where(middle, totals[step - delay], send)
        got = flip(send, axis, 1)
        if step < count:
            part = chunks[step] + got.astype(jnp.float32)
            other = lax.ppermute(part.astype(low), axis, swap)
            totals.append((part + other.astype(jnp.float32)).astype(low))
        if step >= delay:
            results.append(jnp.where(middle, totals[step - delay], got))
    return results


def gather_blocks(own, axis):
    size = lax.axis_size(axis)
    blocks = [own]
    for j in range(1, size):
        top = 1 << (j.bit_length() - 1)
        if j == top:
            blocks.append(flip(own, axis, j))
        elif j & 1:
            blocks.append(flip(blocks[j ^ 1], axis, 1))
        else:
            bottom = j & -j
            first = flip(blocks[j ^ bottom][:1], axis, bottom)
            second = flip(blocks[j ^ top][1:], axis, top)
            blocks.append(jnp.concatenate([first, second], axis=0))
    return blocks


def split_bits(value, bits):
    rows = value.shape[0] >> bits
    return value.reshape((2,) * bits + (rows, value.shape[1]))


def halve(value, axis, order):
    index = lax.axis_index(axis)
    left = sorted(order, reverse=True)
    for bit in order:
        at = left.index(bit)
        side = (index >> bit) & 1
        keep = lax.dynamic_index_in_dim(value, side, at, keepdims=False)
        send = lax.dynamic_index_in_dim(value, 1 - side, at, keepdims=False)
        value = keep + flip(send, axis, 1 << bit)
        left.remove(bit)
    return value


def double(value, axis, order):
    index = lax.axis_index(axis)
    for bit in order:
        side = (index >> bit) & 1
        got = flip(value, axis, 1 << bit)
        low = jnp.where(side == 0, value, got)
        high = jnp.where(side == 0, got, value)
        value = jnp.concatenate([low, high], axis=0)
    return value


def basis_kernel(scale, packed_ref, yre_ref, yim_ref, out_re, out_im, wre, wim, lre, lim):
    order = packed_ref.shape[0]
    row = lax.broadcasted_iota(jnp.int32, (order, order), 0)
    col = lax.broadcasted_iota(jnp.int32, (order, order), 1)
    packed = packed_ref[...]
    turned = packed.T
    wre[...] = jnp.where(row <= col, packed, turned)
    wim[...] = jnp.where(row > col, packed, jnp.where(row < col, -turned, 0.0))
    sub = lax.broadcasted_iota(jnp.int32, (8, order), 0)
    lane = lax.broadcasted_iota(jnp.int32, (8, order), 1)
    sub1 = lax.broadcasted_iota(jnp.int32, (8, 1), 0)
    rows1 = lax.broadcasted_iota(jnp.int32, (order, 8), 0)

    def make_panel(first):
        def panel(p, carry):
            start = pl.multiple_of(p * 8, 8)
            here = lane - start
            block = (here >= 0) & (here < 8)
            pre = wre[pl.ds(start, 8), :]
            pim = wim[pl.ds(start, 8), :]
            bre = [jnp.sum(jnp.where(here == j, pre, 0.0), axis=1, keepdims=True) for j in range(8)]
            bim = [jnp.sum(jnp.where(here == j, pim, 0.0), axis=1, keepdims=True) for j in range(8)]
            pre = jnp.where(block, jnp.where(here == sub, 1.0, 0.0), pre)
            pim = jnp.where(block, 0.0, pim)
            diag = jnp.zeros((8, 1), jnp.float32)
            for i in range(8):
                pivot = bre[i][i : i + 1, :]
                inv = 1.0 / pivot
                diag = jnp.where(sub1 == i, pivot, diag)
                if i == 7:
                    break
                fre = jnp.where(sub1 > i, bre[i] * inv, 0.0)
                fim = jnp.where(sub1 > i, bim[i] * inv, 0.0)
                for j in range(i + 1, 8):
                    tre = bre[j][i : i + 1, :]
                    tim = bim[j][i : i + 1, :]
                    bre[j] = bre[j] - (fre * tre - fim * tim)
                    bim[j] = bim[j] - (fre * tim + fim * tre)
                rre = pre[i : i + 1, :]
                rim = pim[i : i + 1, :]
                pre = pre - (fre * rre - fim * rim)
                pim = pim - (fre * rim + fim * rre)
            dinv = 1.0 / diag
            below = rows1 >= start + 8
            lre[...] = jnp.where(below, (pre * dinv).T, 0.0)
            lim[...] = jnp.where(below, (-pim * dinv).T, 0.0)
            for g in range(first // 8, order // 8):
                rs = pl.ds(g * 8, 8)
                are = jnp.where(block, 0.0, wre[rs, :])
                aim = jnp.where(block, 0.0, wim[rs, :])
                fr = lre[rs, :]
                fi = lim[rs, :]
                for k in range(8):
                    cr = fr[:, k : k + 1]
                    ci = fi[:, k : k + 1]
                    xr = pre[k : k + 1, :]
                    xi = pim[k : k + 1, :]
                    are = are - (cr * xr - ci * xi)
                    aim = aim - (cr * xi + ci * xr)
                wre[rs, :] = are
                wim[rs, :] = aim
            root = scale * lax.rsqrt(diag)
            wre[pl.ds(start, 8), :] = pre * root
            wim[pl.ds(start, 8), :] = pim * root
            return carry

        return panel

    step = 64
    for first in range(0, order, step):
        lax.fori_loop(first // 8, (first + step) // 8, make_panel(first), 0)
    keep = col <= row
    mre = jnp.where(keep, wre[...], 0.0)
    mim = jnp.where(keep, wim[...], 0.0)
    yre = yre_ref[...]
    yim = yim_ref[...]

    def mul(a, b):
        return lax.dot_general(a, b, (((1,), (1,)), ((), ())), precision=HIGH, preferred_element_type=jnp.float32)

    out_re[...] = mul(yre, mre) + mul(yim, mim)
    out_im[...] = mul(yim, mre) - mul(yre, mim)


def basis(packed, yre, yim, scale):
    order = packed.shape[0]
    shape = jax.ShapeDtypeStruct(yre.shape, jnp.float32)
    square = pltpu.VMEM((order, order), jnp.float32)
    slim = pltpu.VMEM((order, 8), jnp.float32)
    return pl.pallas_call(
        functools.partial(basis_kernel, scale),
        out_shape=(shape, shape),
        scratch_shapes=[square, square, slim, slim],
        name="basis",
    )(packed, yre, yim)


def permute_columns(reflection, element_order):
    panels = reflection.shape[2] // PANEL_W
    natural = jnp.arange(PANEL_W, dtype=jnp.int32)
    flat = reflection.reshape(-1, reflection.shape[2])
    pieces = []
    for k in range(panels):
        part = slice(k * PANEL_W, (k + 1) * PANEL_W)
        picks = (element_order[part, None] % PANEL_W == natural[None, :]).astype(jnp.bfloat16)
        pieces.append(dot(flat[:, part], picks).astype(jnp.bfloat16))
    return jnp.concatenate(pieces, axis=1).reshape(reflection.shape)


def body(reflection, focus_in, focus_out, ref_angle, element_order, q_start):
    cols = lax.axis_size("col")
    bits = cols.bit_length() - 1
    index = lax.axis_index("col")
    blocks = gather_blocks(permute_columns(reflection, element_order), "col")
    odd = index & 1
    partials = []
    for k in range(cols // 2):
        first = jnp.where(odd == 0, blocks[2 * k], blocks[2 * k + 1])
        second = jnp.where(odd == 0, blocks[2 * k + 1], blocks[2 * k])
        pair = jnp.concatenate([first, second], axis=1)
        partials.extend(cross(pair[0], pair[1], focus_in[0], focus_in[1]))
    summed = line_sum(partials, "row", 3)
    pair_rows = summed[0].shape[0]
    focus_re = jnp.zeros((pair_rows * cols // 2, focus_in.shape[2]), jnp.bfloat16)
    focus_im = focus_re
    for k in range(cols // 2):
        at = ((index >> 1) ^ k) * pair_rows
        focus_re = lax.dynamic_update_slice_in_dim(focus_re, summed[2 * k], at, 0)
        focus_im = lax.dynamic_update_slice_in_dim(focus_im, summed[2 * k + 1], at, 0)
    cosine = jnp.cos(ref_angle)
    sine = jnp.sin(ref_angle)
    width = focus_in.shape[2] // FOCAL_CHUNKS
    dense = []
    starts = []
    for k in range(FOCAL_CHUNKS):
        part = slice(k * width, (k + 1) * width)
        outer_re, outer_im = cross(focus_out[0], focus_out[1], focus_re[:, part], focus_im[:, part])
        dense_re = (outer_re * cosine[:, part] + outer_im * sine[:, part]).astype(jnp.bfloat16)
        dense_im = (outer_im * cosine[:, part] - outer_re * sine[:, part]).astype(jnp.bfloat16)
        adj_re, adj_im = adjoint_product(dense_re, dense_im, q_start[:, 0], q_start[:, 1])
        dense.append((dense_re, dense_im))
        starts.append(jnp.concatenate([adj_re, adj_im], axis=1))
    adjoint = line_sum(starts, "row", 3)
    rank = q_start.shape[2]
    image_re = image_im = 0.0
    for (dense_re, dense_im), adj in zip(dense, adjoint):
        more_re, more_im = cross(dense_re, dense_im, adj[:, :rank], adj[:, rank:])
        image_re = image_re + more_re
        image_im = image_im + more_im
    ups = list(range(bits))
    image_re = halve(split_bits(image_re, bits), "col", ups)
    image_im = halve(split_bits(image_im, bits), "col", ups[:1] + ups[1:][::-1])
    gram_re, gram_im = adjoint_product(image_re, image_im, image_re, image_im, HIGH)
    upper = lax.broadcasted_iota(jnp.int32, gram_re.shape, 0) <= lax.broadcasted_iota(jnp.int32, gram_re.shape, 1)
    packed = jnp.where(upper, gram_re, gram_im)
    share = halve(split_bits(packed, bits), "col", ups)
    others = [flip(share, "row", mask) for mask in range(1, lax.axis_size("row"))]
    share = share + sum(others)
    packed = double(share, "col", ups)
    scale = math.sqrt(ref_angle.shape[0] * lax.axis_size("row"))
    basis_re, basis_im = basis(packed, image_re, image_im, scale)
    return jnp.stack([basis_re, basis_im], axis=1)


def solution(mesh):
    in_specs = (
        P(None, "col", "row"),
        P(None, "row", "col"),
        P(None, "row", None),
        P("row", "col"),
        P("row"),
        P("row", None, None),
    )
    out_specs = P(("row", "col"), None, None)
    return jax.shard_map(body, mesh=mesh, in_specs=in_specs, out_specs=out_specs, check_vma=False)
```
